512 devices in a mesh: groups: 2 (over y), seq: 32 (over z, core), head: 8 (over x).
Axes of the slice: x: 8, y: 2, z: 16, core: 2. Of those that a mesh axis runs over, the one named last changes fastest.
The devices are a block of a 8x8x16 slice.
Arguments:
- queries: bfloat16 [12288, 16, 576], P(('groups', 'seq'), 'head'), parts along dimension 0, may hold values from -40 to 40
- latent_kv: bfloat16 [12288, 576], P(('groups', 'seq')), parts along dimension 0, may hold values from -6 to 6
- adapter_ids: int32 [384], P(('groups', 'seq')), parts along dimension 0, may hold values from 0 to 4
- value_up: bfloat16 [16, 512, 128], P('head'), may hold values from -0.25 to 0.25
- output_weight: bfloat16 [2048, 2048], P('head'), may hold values from -0.1875 to 0.1875
- adapter_down: bfloat16 [2048, 80], P('head'), may hold values from -0.125 to 0.125
- adapter_up: bfloat16 [80, 2048], replicated, may hold values from -1.5 to 1.5
Outputs:
- mixed: bfloat16 [12288, 2048], P(('groups', 'seq'), 'head'), parts along dimension 0
The draws below stay inside these ranges and needn't reach their ends.
There are 2 independent parts, one for each index of `groups`. The reference program is written for one: setup_inputs(seed, part) draws one part's arguments, and reference() takes and returns one part's arrays. A program takes and returns all parts, laid end to end along the dimension named above; an argument that names none is the same for every part. Nothing has to cross between parts.
All inputs are finite; a program needn't handle non-finite values.
Results may differ from the reference program's by a relative error of at most 0.017.
Values may be sent and summed in bfloat16 or wider, within the bound.
A program may use at most 64 MiB of HBM per device.

```python
import math
import jax
import jax.numpy as jnp
from jax import lax

D = 2048
HEADS = 16
LATENT = 512
ROPE = 64
NOPE = 128
VHEAD = 128
ADAPTERS = 5
RANK = 16
ADP_BLOCK = 32
TOK_DEV = 192
TOKENS = 6144
N_SEQ = 32


def pair_draws(key):
    base = jax.random.fold_in(key, 11)
    first_key, second_key = jax.random.split(base, 2)
    latent_width = LATENT + ROPE
    latent = jnp.clip(jax.random.normal(first_key, (TOKENS, latent_width), jnp.float32), -6.0, 6.0)
    queries = jnp.clip(jax.random.normal(second_key, (TOKENS, HEADS, latent_width), jnp.float32), -6.0, 6.0)
    queries = jnp.clip(queries, -40.0, 40.0)
    return (latent, queries)


def draw_latent_kv(key, part):
    return pair_draws(key)[0].astype(jnp.bfloat16)


def draw_queries(key, part):
    return pair_draws(key)[1].astype(jnp.bfloat16)


def place_ends(result, stream_key, smallest, high):
    spot = [jax.random.randint(jax.random.fold_in(stream_key, axis), (), 0, length) for axis, length in enumerate(result.shape)]
    main_axis = result.shape.index(max(result.shape))
    beside = spot[:main_axis] + [(spot[main_axis] + 1) % result.shape[main_axis]] + spot[main_axis + 1:]
    return result.at[tuple(spot)].set(smallest).at[tuple(beside)].set(high)


def spiked(entries, own_key, source, target, shards_of, factor):
    owner, partner = [(jnp.arange(entries.shape[dim]) // (entries.shape[dim] // shards_of)).reshape([-1 if axis == dim else 1 for axis in range(entries.ndim)]) for dim in (source, target)]
    chosen = jax.random.permutation(own_key, shards_of)[partner]
    strong = (owner == chosen) | (owner == (partner + shards_of // 2) % shards_of)
    return jnp.where(strong, factor * entries, entries)


def level_of(stream_key, dims, cuts, low, high):
    def one(dim, parts):
        steps = jax.random.uniform(jax.random.fold_in(jax.random.fold_in(stream_key, 6), dim), (parts,), jnp.float32, low / len(cuts), high / len(cuts))
        return jnp.repeat(jnp.exp(steps), dims[dim] // parts).reshape((-1,) + (1,) * (len(dims) - dim - 1))

    loudness = one(*cuts[0])
    for cut in cuts[1:]:
        loudness = loudness * one(*cut)
    return loudness


def scatter_about(own_key, dims, width, reach, shards=(), held_as=jnp.bfloat16):
    array = jax.random.normal(own_key, dims, jnp.float32) * width
    if len(shards) > 0:
        array = level_of(own_key, dims, shards, -0.22, 0.18) * array
    return jnp.clip(array, min=-reach, max=reach).astype(held_as)


def noise_with(rng, extent, spread, reach, pieces, heavy, kind=jnp.bfloat16):
    result = spread * jax.random.normal(rng, extent, jnp.float32)
    if pieces:
        result = result * level_of(rng, extent, pieces, -0.22, 0.18)
    return jnp.clip(spiked(result, jax.random.fold_in(rng, 3), *heavy), -reach, reach).astype(kind)


def setup_inputs(seed: int = 0, part: int = 0) -> dict:
    seeds = jax.random.split(jax.random.key(seed), 8)
    part_splits = jax.random.split(jax.random.fold_in(seeds[7], part), 8)
    queries = draw_queries(jax.random.fold_in(jax.random.fold_in(seeds[7], part), 71), part)
    latent_kv = draw_latent_kv(jax.random.fold_in(jax.random.fold_in(seeds[7], part), 71), part)
    adapter_ids = place_ends(jax.random.randint(part_splits[2], (TOKENS // ADP_BLOCK,), 0, ADAPTERS), jax.random.fold_in(part_splits[2], 1), 0, ADAPTERS - 1).astype(jnp.int32)
    value_up = scatter_about(seeds[3], (HEADS, LATENT, VHEAD), LATENT ** -0.5, 0.25, ((0, 8),))
    output_weight = noise_with(seeds[4], (HEADS * VHEAD, D), (HEADS * VHEAD) ** -0.5, 0.1875, ((0, 8),), (0, 1, 8, 2.0))
    adapter_down = scatter_about(seeds[5], (HEADS * VHEAD, ADAPTERS * RANK), (HEADS * VHEAD) ** -0.5, 0.125, ((0, 8),))
    adapter_up = scatter_about(seeds[6], (ADAPTERS * RANK, D), RANK ** -0.5, 1.5)
    return dict(queries=queries, latent_kv=latent_kv, adapter_ids=adapter_ids, value_up=value_up, output_weight=output_weight, adapter_down=adapter_down, adapter_up=adapter_up)


def mirror_position(rows, tok_dev, count):
    shard = rows // tok_dev
    within = rows % tok_dev
    half = tok_dev // 2
    return jnp.where(within < half, shard * half + within, (2 * count - 1 - shard) * half + within - half).astype(jnp.int32)

def reference(queries, latent_kv, adapter_ids, value_up, output_weight, adapter_down, adapter_up):
    score_scale = 1.0 / math.sqrt(NOPE + ROPE)
    position = mirror_position(jnp.arange(TOKENS, dtype=jnp.int32), TOK_DEV, N_SEQ)
    visible = position[None, :] <= position[:, None]
    latent = latent_kv[:, :LATENT]

    def one_head(index):
        query = lax.dynamic_index_in_dim(queries, index, 1, keepdims=False)
        scores = lax.dot_general(query, latent_kv, (((1,), (1,)), ((), ())), preferred_element_type=jnp.float32) * score_scale
        scores = jnp.where(visible, scores, -1e+30)
        row_max = lax.optimization_barrier(jnp.max(scores, axis=1, keepdims=True))
        weights = jnp.exp(scores - row_max)
        row_sum = lax.optimization_barrier(jnp.sum(weights, axis=1, keepdims=True))
        latent_out = jnp.dot(weights.astype(jnp.bfloat16), latent, preferred_element_type=jnp.float32) / row_sum
        return latent_out.astype(jnp.bfloat16)
    latent_out = lax.map(one_head, jnp.arange(HEADS, dtype=jnp.int32))
    value_out = jnp.einsum('hsl,hlv->shv', latent_out.astype(jnp.float32), value_up.astype(jnp.float32))
    value_out = value_out.astype(jnp.bfloat16).reshape(TOKENS, HEADS * VHEAD)
    projected = jnp.dot(value_out, output_weight, preferred_element_type=jnp.float32)
    rank_terms = jnp.dot(value_out, adapter_down, preferred_element_type=jnp.float32)
    token_ids = jnp.repeat(adapter_ids, ADP_BLOCK, total_repeat_length=TOKENS)
    owner = jnp.arange(ADAPTERS * RANK, dtype=jnp.int32) // RANK
    selector = (token_ids[:, None] == owner[None, :]).astype(jnp.float32)
    adapted = jnp.dot(rank_terms * selector, adapter_up.astype(jnp.float32), precision=lax.Precision.HIGHEST)
    return (projected + adapted).astype(jnp.bfloat16)
```

```python
import functools
import math

import jax
import jax.numpy as jnp
from jax import lax
from jax.experimental import pallas as pl
from jax.experimental.pallas import tpu as pltpu
from jax.sharding import PartitionSpec as P

ROPE = 64
NOPE = 128
ADAPTERS = 5
RANK = 16
ADP_BLOCK = 32
UNIT = 16
BF16 = jnp.bfloat16
F32 = jnp.float32
MESH = pl.DeviceIdType.MESH


def kernel(
    cfg,
    ids_ref,
    q_hbm,
    kv_ref,
    vup_hbm,
    w_hbm,
    down_hbm,
    up_hbm,
    out_ref,
    buf,
    q_ref,
    vup_ref,
    w_ref,
    down_ref,
    up_ref,
    m_ref,
    l_ref,
    acc_ref,
    part_ref,
    sum_ref,
    rs_ref,
    load_sem,
    send_sem,
    z_sem,
    x_sem,
    c_sem,
    rs_send,
    rs_sem,
):
    rows_z, n_x, half, latent, vhead = cfg
    pack = half // 2
    units = pack // UNIT
    reach = rows_z // 2
    wide = 2 * latent
    scale = math.log2(math.e) / math.sqrt(NOPE + ROPE)
    heads = q_ref.shape[1] // half
    nodes = 2 * rows_z

    seq = lax.axis_index("seq")
    x = lax.axis_index("head")
    z, core = seq // 2, seq % 2
    sigma = 1 - 2 * core
    parity = x % 2

    def row(delta):
        return (z + delta + 2 * rows_z) % rows_z

    def col(delta):
        return (x + delta + 2 * n_x) % n_x

    def chunk(zz, cc, late):
        s = 2 * zz + cc
        return s + late * (2 * nodes - 1 - 2 * s)

    ahead = {"seq": 2 * row(sigma) + core}
    behind = {"seq": 2 * row(-sigma) + core}
    sibling = {"seq": 2 * z + 1 - core}
    x_ahead = {"head": col(sigma)}
    x_behind = {"head": col(-sigma)}

    loads = [
        pltpu.make_async_copy(src, dst, load_sem.at[i])
        for i, (src, dst) in enumerate(
            (
                (q_hbm, q_ref),
                (vup_hbm, vup_ref),
                (w_hbm, w_ref),
                (down_hbm, down_ref),
                (up_hbm, up_ref),
            )
        )
    ]
    for load in loads:
        load.start()

    for late in (0, 1):
        own = kv_ref[late * half : (late + 1) * half, :]
        first, second = own[:pack], own[pack:]
        c = chunk(z, core, late)
        buf[c, :, :latent] = first[:, :latent]
        buf[c, :, latent:wide] = second[:, :latent]
        buf[c, :, wide:] = jnp.concatenate([first[:, latent:], second[:, latent:]], axis=1)

    barrier = pltpu.get_barrier_semaphore()
    pl.semaphore_signal(barrier, inc=1, device_id=sibling, device_id_type=MESH)
    for peer in (ahead, behind, x_ahead, x_behind):
        pl.semaphore_signal(barrier, inc=1, device_id=peer, device_id_type=MESH)
    pl.semaphore_wait(barrier, 5)

    def push(ref, send, recv, peer):
        pltpu.make_async_remote_copy(
            src_ref=ref, dst_ref=ref, send_sem=send, recv_sem=recv, device_id=peer, device_id_type=MESH
        ).start()

    def arrived(ref, recv):
        pltpu.make_async_copy(ref, ref, recv).wait()

    def unit(c, j):
        return buf.at[c, pl.ds(j * UNIT, UNIT)]

    AHEAD, BEHIND, XA, XB, SIB = range(5)

    own = chunk(z, core, parity)
    for j in range(units):
        push(unit(own, j), send_sem.at[AHEAD], z_sem.at[z, j], ahead)
        push(unit(own, j), send_sem.at[BEHIND], z_sem.at[z, j], behind)
    for late in (0, 1):
        push(buf.at[chunk(z, core, late)], send_sem.at[SIB], c_sem.at[z, late], sibling)

    def from_z(zz, j, onward, slot):
        c = chunk(zz, core, parity)
        piece = unit(c, j)
        arrived(piece, z_sem.at[zz, j])
        if onward is not None:
            push(piece, send_sem.at[slot], z_sem.at[zz, j], onward)
        if j == 0:
            push(piece, send_sem.at[XB], x_sem.at[zz, j], x_behind)
        else:
            push(piece, send_sem.at[XA], x_sem.at[zz, j], x_ahead)
        push(piece, send_sem.at[SIB], c_sem.at[zz, parity], sibling)

    def from_x(zz, j):
        piece = unit(chunk(zz, core, 1 - parity), j)
        arrived(piece, x_sem.at[zz, j])
        push(piece, send_sem.at[SIB], c_sem.at[zz, 1 - parity], sibling)

    def from_sibling(zz):
        for late in (0, 1):
            arrived(buf.at[chunk(zz, 1 - core, late)], c_sem.at[zz, late])

    def keys(base):
        pair = buf[pl.ds(base, 2)].reshape(2 * pack, wide + 2 * ROPE)
        value = jnp.concatenate([pair[:, :latent], pair[:, latent:wide]], axis=0)
        turned = jnp.concatenate([pair[:, wide : wide + ROPE], pair[:, wide + ROPE :]], axis=0)
        return value, turned

    def attend(which, bases, mask_shift=None, first=False):
        got = [keys(b) for b in bases]
        value = jnp.concatenate([g[0] for g in got], axis=0) if len(got) > 1 else got[0][0]
        turned = jnp.concatenate([g[1] for g in got], axis=0) if len(got) > 1 else got[0][1]
        nt = (((1,), (1,)), ((), ()))
        s = lax.dot_general(
            q_ref[which, :, :latent], value, nt, preferred_element_type=F32
        ) + lax.dot_general(q_ref[which, :, latent:], turned, nt, preferred_element_type=F32)
        if mask_shift is not None:
            n = lax.broadcasted_iota(jnp.int32, s.shape, 1)
            i = lax.broadcasted_iota(jnp.int32, s.shape, 0) % half
            at = ((n % (2 * pack)) // pack) * half + (n // (2 * pack)) * pack + n % pack
            s = jnp.where(at <= i + mask_shift, s, -1e30)
        top = jnp.max(s, axis=1, keepdims=True)
        if first:
            m = top
        else:
            old = m_ref[which][:, :1]
            m = jnp.maximum(old, top)
            decay = jnp.exp2((old - m) * scale)
        w = jnp.exp2((s - m) * scale)
        total = jnp.sum(w, axis=1, keepdims=True)
        new = jnp.dot(w.astype(BF16), value, preferred_element_type=F32)
        if not first:
            total = total + l_ref[which][:, :1] * decay
            new = new + acc_ref[which] * decay
        m_ref[which] = jnp.broadcast_to(m, m_ref.shape[1:])
        l_ref[which] = jnp.broadcast_to(total, l_ref.shape[1:])
        acc_ref[which] = new

    def low(zz):
        return 2 * zz

    def high(zz):
        return 2 * nodes - 2 - 2 * zz

    def extra(t, sign):
        raw = z + sign * t
        zz = (raw + rows_z) % rows_z
        before = jnp.where(zz < z, 1, 0)
        attend(1 - before, [low(zz) + (1 - before) * (high(zz) - low(zz))])

    def compute(t):
        from_sibling(row(-t))
        from_sibling(row(t))
        attend(1, [low(row(-t)), low(row(t))])
        extra(t, -1)
        extra(t, 1)

    def step_z(t, last_behind=False):
        for j in range(units):
            from_z(row(-sigma * t), j, ahead, AHEAD)
            from_z(row(sigma * t), j, None if last_behind else behind, BEHIND)

    def step_x(t):
        for j in range(units):
            from_x(row(-sigma * t), j)
            from_x(row(sigma * t), j)

    loads[0].wait()
    from_sibling(z)
    attend(1, [high(z)], mask_shift=(1 - core) * half, first=True)
    attend(0, [low(z)], mask_shift=core * half, first=True)
    attend(1, [low(z)])

    step_z(1)
    step_z(2)
    step_x(1)

    def body(t, carry):
        step_z(t)
        step_x(t - 1)
        compute(t - 2)
        return carry

    lax.fori_loop(3, reach - 1, body, 0)
    step_z(reach - 1, last_behind=True)
    step_x(reach - 2)
    compute(reach - 3)
    far = row(reach)
    for j in range(units):
        from_z(far, j, None, None)
    step_x(reach - 1)
    compute(reach - 2)
    for j in range(units):
        from_x(far, j)
    compute(reach - 1)
    from_sibling(far)
    attend(1, [low(far)])
    before = jnp.where(far < z, 1, 0)
    attend(1 - before, [low(far) + (1 - before) * (high(far) - low(far))])

    for load in loads[1:]:
        load.wait()

    features = w_ref.shape[1]
    share = features // n_x

    def project(which):
        o = acc_ref[which] * (1.0 / l_ref[which][:, :1])
        o = o.astype(BF16)
        vo = jnp.concatenate(
            [
                jnp.dot(o[h * half : (h + 1) * half], vup_ref[h], preferred_element_type=F32).astype(BF16)
                for h in range(heads)
            ],
            axis=1,
        )
        rank = jnp.dot(vo, down_ref[...], preferred_element_type=F32)
        r = lax.broadcasted_iota(jnp.int32, rank.shape, 0) // ADP_BLOCK
        owner = lax.broadcasted_iota(jnp.int32, rank.shape, 1) // RANK
        blocks = half // ADP_BLOCK
        pick = jnp.zeros(rank.shape, jnp.int32)
        for b in range(blocks):
            pick = jnp.where(r == b, ids_ref[which * blocks + b], pick)
        chosen = jnp.where(owner == pick, rank, 0.0)
        hi = chosen.astype(BF16)
        rest = chosen - hi.astype(F32)
        mid = rest.astype(BF16)
        lo = (rest - mid.astype(F32)).astype(BF16)
        for d in range(n_x):
            cols = slice(d * share, (d + 1) * share)
            up = up_ref[:, cols]
            y = jnp.dot(vo, w_ref[:, cols], preferred_element_type=F32)
            y = y + (
                jnp.dot(hi, up, preferred_element_type=F32)
                + jnp.dot(mid, up, preferred_element_type=F32)
                + jnp.dot(lo, up, preferred_element_type=F32)
            )
            part_ref[which, d] = y.astype(BF16)

    far_x = n_x // 2

    def rs_push(ref, which, way, k):
        pltpu.make_async_remote_copy(
            src_ref=ref,
            dst_ref=rs_ref.at[which, way, k],
            send_sem=rs_send.at[way],
            recv_sem=rs_sem.at[which, way, k],
            device_id=x_ahead if way == 0 else x_behind,
            device_id_type=MESH,
        ).start()

    for which in (0, 1):
        project(which)
        rs_push(part_ref.at[which, col(sigma * far_x)], which, 0, 0)
        rs_push(part_ref.at[which, col(-sigma * (far_x - 1))], which, 1, 0)

    for k in range(1, far_x):
        for which in (0, 1):
            for way in (0, 1):
                hops = far_x - way - k
                if hops < 1:
                    continue
                arrived(rs_ref.at[which, way, k - 1], rs_sem.at[which, way, k - 1])
                dest = col((sigma if way == 0 else -sigma) * hops)
                sum_ref[which, way, k] = (
                    rs_ref[which, way, k - 1].astype(F32) + part_ref[which, dest].astype(F32)
                ).astype(BF16)
                rs_push(sum_ref.at[which, way, k], which, way, k)

    for which in (0, 1):
        for way in (0, 1):
            k = far_x - 1 - way
            arrived(rs_ref.at[which, way, k], rs_sem.at[which, way, k])
        out_ref[which * half : (which + 1) * half, :] = (
            part_ref[which, x].astype(F32)
            + rs_ref[which, 0, far_x - 1].astype(F32)
            + rs_ref[which, 1, far_x - 2].astype(F32)
        ).astype(BF16)

    def drained(ref, sem):
        pltpu.make_async_copy(ref, ref, sem).wait()

    others = rows_z - 1
    drained(buf.at[pl.ds(0, reach)], send_sem.at[AHEAD])
    drained(buf.at[pl.ds(0, reach - 1)], send_sem.at[BEHIND])
    drained(buf.at[pl.ds(0, others), pl.ds(0, UNIT)], send_sem.at[XB])
    drained(buf.at[pl.ds(0, others), pl.ds(0, pack - UNIT)], send_sem.at[XA])
    drained(buf.at[pl.ds(0, 2 * rows_z)], send_sem.at[SIB])
    for way in (0, 1):
        drained(rs_ref.at[:, way, pl.ds(0, far_x - way)], rs_send.at[way])


def body(n_seq, n_x, queries, latent_kv, adapter_ids, value_up, output_weight, adapter_down, adapter_up):
    tok, heads, width = queries.shape
    latent, vhead = value_up.shape[1:]
    half = tok // 2
    q = queries.reshape(2, half, heads, width).swapaxes(1, 2).reshape(2, heads * half, width)
    features = output_weight.shape[1]
    share = features // n_x
    rows_z = n_seq // 2
    far_x = n_x // 2
    pack = half // 2
    any_spec = pl.BlockSpec(memory_space=pl.ANY)
    vmem = pl.BlockSpec(memory_space=pltpu.VMEM)
    return pl.pallas_call(
        functools.partial(kernel, (rows_z, n_x, half, latent, vhead)),
        out_shape=jax.ShapeDtypeStruct((tok, share), BF16),
        in_specs=[pl.BlockSpec(memory_space=pltpu.SMEM), any_spec, vmem, any_spec, any_spec, any_spec, any_spec],
        out_specs=vmem,
        scratch_shapes=[
            pltpu.VMEM((2 * n_seq, pack, 2 * width), BF16),
            pltpu.VMEM(q.shape, BF16),
            pltpu.VMEM(value_up.shape, BF16),
            pltpu.VMEM(output_weight.shape, BF16),
            pltpu.VMEM(adapter_down.shape, BF16),
            pltpu.VMEM(adapter_up.shape, BF16),
            pltpu.VMEM((2, heads * half, 128), F32),
            pltpu.VMEM((2, heads * half, 128), F32),
            pltpu.VMEM((2, heads * half, latent), F32),
            pltpu.VMEM((2, n_x, half, share), BF16),
            pltpu.VMEM((2, 2, far_x, half, share), BF16),
            pltpu.VMEM((2, 2, far_x, half, share), BF16),
            pltpu.SemaphoreType.DMA((5,)),
            pltpu.SemaphoreType.DMA((5,)),
            pltpu.SemaphoreType.DMA((rows_z, pack // UNIT)),
            pltpu.SemaphoreType.DMA((rows_z, pack // UNIT)),
            pltpu.SemaphoreType.DMA((rows_z, 2)),
            pltpu.SemaphoreType.DMA((2,)),
            pltpu.SemaphoreType.DMA((2, 2, far_x)),
        ],
        compiler_params=pltpu.CompilerParams(
            collective_id=0, has_side_effects=True, vmem_limit_bytes=56 * 1024 * 1024
        ),
    )(adapter_ids, q, latent_kv, value_up, output_weight, adapter_down, adapter_up)


def solution(mesh):
    return jax.shard_map(
        functools.partial(body, mesh.shape["seq"], mesh.shape["head"]),
        mesh=mesh,
        in_specs=(
            P(("groups", "seq"), "head", None),
            P(("groups", "seq"), None),
            P(("groups", "seq")),
            P("head", None, None),
            P("head", None),
            P("head", None),
            P(),
        ),
        out_specs=P(("groups", "seq"), "head"),
        check_vma=False,
    )
```
